32 devices in a mesh: trial: 4 (over z), south: 2 (over core), east: 2 (over x), down: 2 (over y).
Axes of the slice: x: 2, y: 2, z: 4, core: 2. Of those that a mesh axis runs over, the one named last changes fastest.
Arguments:
- tracer: float32 [32, 32, 256, 128], P(('trial', 'south'), 'east', 'down'), parts along dimension 0, may hold values from 0.5 to 2
- mobility: float32 [32, 32, 256, 128], P(('trial', 'south'), 'east', 'down'), parts along dimension 0, may hold values from 0.03 to 0.15
- source: float32 [32, 32, 256, 128], P(('trial', 'south'), 'east', 'down'), parts along dimension 0, may hold values from -0.2 to 0.2
Outputs:
- standardized: float32 [32, 32, 256, 128], P(('trial', 'south'), 'east', 'down'), parts along dimension 0
- tracer_end: float32 [32, 32, 256, 128], P(('trial', 'south'), 'east', 'down'), parts along dimension 0
The draws below stay inside these ranges and needn't reach their ends.
There are 4 independent parts, one for each index of `trial`. The reference program is written for one: setup_inputs(seed, part) draws one part's arguments, and reference() takes and returns one part's arrays. A program takes and returns all parts, laid end to end along the dimension named above; each array names one. Nothing has to cross between parts.
All inputs are finite; a program needn't handle non-finite values.
Results may differ from the reference program's by a relative error of at most 0.00002.
Values sent between devices are 32-bit elements; how exact they have to be, the bound alone decides.
A program may use at most 128 MiB of HBM per device.

```python
import jax
import jax.numpy as jnp
from jax import lax

GRID_Y = 8
GRID_X = 32
GRID_Z = 256
LEVELS = 128
STEPS = 3


def level_of(stream_key, shape, split, least, top_value):
    level = 1.0
    for axis_at, shards_of in split:
        heights = jax.random.uniform(jax.random.fold_in(jax.random.fold_in(stream_key, 6), axis_at), (shards_of,), jnp.float32, least / len(split), top_value / len(split))
        level = level * jnp.repeat(jnp.exp(heights), shape[axis_at] // shards_of).reshape((-1,) + (1,) * (len(shape) - 1 - axis_at))
    return level


def setup_inputs(seed: int = 0, part: int = 0) -> dict:
    arg_keys = jax.random.split(jax.random.key(seed), 4)
    part_keys = jax.random.split(jax.random.fold_in(arg_keys[3], part), 4)
    tracer = jnp.clip(0.5 + 1.5 * jax.random.uniform(part_keys[0], (GRID_Y, GRID_X, GRID_Z, LEVELS), jnp.float32) ** level_of(part_keys[0], (GRID_Y, GRID_X, GRID_Z, LEVELS), ((0, 2), (1, 2), (2, 2)), -0.2, 0.2), 0.5, 2.0)
    mobility = jnp.clip(0.03 + 0.120000007 * jax.random.uniform(part_keys[1], (GRID_Y, GRID_X, GRID_Z, LEVELS), jnp.float32) ** level_of(part_keys[1], (GRID_Y, GRID_X, GRID_Z, LEVELS), ((0, 2), (1, 2), (2, 2)), -0.2, 0.2), 0.03, 0.15)
    source = jnp.clip(jax.random.uniform(part_keys[2], (GRID_Y, GRID_X, GRID_Z, LEVELS), jnp.float32, -0.2, 0.2) * level_of(part_keys[2], (GRID_Y, GRID_X, GRID_Z, LEVELS), ((0, 2), (1, 2), (2, 2)), -0.4, 0.0), -0.2, 0.2)
    return dict(tracer=tracer, mobility=mobility, source=source)


def strip_edges(values, dims):
    for dim in dims:
        values = lax.slice_in_dim(values, 1, values.shape[dim] - 1, axis=dim)
    return values

def neighbour(values, dim, start, dims):
    others = [other for other in dims if other != dim]
    values = strip_edges(values, others)
    return lax.slice_in_dim(values, start, start + values.shape[dim] - 2, axis=dim)

def one_step(padded, mobility, source):
    middle = strip_edges(padded, (0, 1, 2))
    lower = [neighbour(padded, dim, 0, (0, 1, 2)) for dim in (0, 1, 2)]
    upper = [neighbour(padded, dim, 2, (0, 1, 2)) for dim in (0, 1, 2)]
    spread = lower[0] + upper[0] + lower[1] + upper[1] + lower[2] + upper[2] - 6.0 * middle
    return middle + mobility * spread + source

def reference(tracer, mobility, source):
    for step in range(STEPS):
        tracer = one_step(jnp.pad(tracer, ((1, 1), (1, 1), (1, 1), (0, 0)), mode='wrap'), mobility, source)
    line_mean = lax.optimization_barrier(jnp.mean(tracer, axis=2, keepdims=True))
    centred = tracer - line_mean
    line_variance = lax.optimization_barrier(jnp.mean(centred * centred, axis=2, keepdims=True))
    standardized = centred * lax.rsqrt(line_variance + 0.0001)
    return (standardized, tracer)
```

```python
import functools

import jax
import jax.numpy as jnp
from jax import lax
from jax.experimental import pallas as pl
from jax.experimental.pallas import tpu as pltpu
from jax.sharding import PartitionSpec as P

MESH = pl.DeviceIdType.MESH
PAD = 8
ROWS = 32
EPS = 0.0001


def kernel(
    counts, tracer, mobility, source, standardized, end,
    t0, t1, t2, mob, src, stats,
    load_sem, x_send, x_recv, y_send, y_recv, z_send, z_recv, s_send, s_recv,
):
    ny, nx, nz, _ = mob.shape
    n_down = counts["down"]
    me = {axis: lax.axis_index(axis) for axis in counts}

    def peer(axis, offset):
        count = counts[axis]
        return {axis: lax.rem(me[axis] + (offset % count), count)}

    fields = (t0, t1, t2)
    line = pl.ds(PAD, nz)
    low, high, middle = (pl.ds(1, 1), pl.ds(nx, 1), pl.ds(2, nx - 2))
    groups = (middle, low, high)

    def load(sem, array, into):
        return pltpu.make_async_copy(array, into, load_sem.at[sem])

    def load_field(sem, columns):
        inside = pl.ds(columns.start - 1, columns.size)
        return load(sem, tracer.at[:, inside], t0.at[pl.ds(1, ny), columns, line])

    loads = [load_field(i, c) for i, c in enumerate((low, high, middle))]
    loads += [load(3, mobility, mob), load(4, source, src)]
    for copy in loads:
        copy.start()

    def send(field, from_, to, sems, at, device):
        return pltpu.make_async_remote_copy(
            src_ref=field.at[from_],
            dst_ref=field.at[to],
            send_sem=sems[0].at[at],
            recv_sem=sems[1].at[at],
            device_id=device,
            device_id_type=MESH,
        )

    inner_y = pl.ds(1, ny)

    def face(step, side):
        from_, to, offset = ((1, nx + 1, -1), (nx, 0, 1))[side]
        return send(
            fields[step],
            (inner_y, pl.ds(from_, 1), line),
            (inner_y, pl.ds(to, 1), line),
            (x_send, x_recv), (step, side), peer("east", offset),
        )

    def borders(step, group):
        columns = groups[group]
        field = fields[step]
        copies = []
        for side, (from_, to, offset) in enumerate(((1, ny + 1, -1), (ny, 0, 1))):
            copies.append(send(
                field, (pl.ds(from_, 1), columns, line), (pl.ds(to, 1), columns, line),
                (y_send, y_recv), (step, side, group), peer("south", offset),
            ))
        for side, (from_, to, offset) in enumerate(
            ((PAD, PAD + nz, -1), (PAD + nz - 1, PAD - 1, 1))
        ):
            copies.append(send(
                field, (inner_y, columns, pl.ds(from_, 1)), (inner_y, columns, pl.ds(to, 1)),
                (z_send, z_recv), (step, side, group), peer("down", offset),
            ))
        return copies

    def moments(group):
        columns = groups[group]
        inside = pl.ds(columns.start - 1, columns.size)
        return [
            pltpu.make_async_remote_copy(
                src_ref=stats.at[0, inside],
                dst_ref=stats.at[j, inside],
                send_sem=s_send.at[j - 1, group],
                recv_sem=s_recv.at[j - 1, group],
                device_id=peer("down", j),
                device_id_type=MESH,
            )
            for j in range(1, n_down)
        ]

    started = []

    def start(copies):
        for copy in copies:
            copy.start()
            started.append(copy)

    barrier = pltpu.get_barrier_semaphore()
    greeted = [peer("south", -1), peer("south", 1), peer("east", -1), peer("east", 1)]
    greeted += [peer("down", j) for j in range(1, n_down)]
    for device in greeted:
        pl.semaphore_signal(barrier, inc=1, device_id=device, device_id_type=MESH)
    pl.semaphore_wait(barrier, len(greeted))

    faces = [[face(step, side) for side in (0, 1)] for step in range(3)]
    edges = [[borders(step, group) for group in range(3)] for step in range(3)]
    spread_moments = [moments(group) for group in range(3)]

    def column(step, x):
        field = fields[step]
        for z in range(0, nz, ROWS):
            at = pl.ds(PAD + z, ROWS)
            before, after = pl.ds(PAD + z - 1, ROWS), pl.ds(PAD + z + 1, ROWS)
            rows = pl.ds(z, ROWS)
            lines = [field[y, x, at] for y in range(ny + 2)]
            for y in range(1, ny + 1):
                mid = lines[y]
                total = lines[y - 1] + lines[y + 1]
                total += field[y, x - 1, at] + field[y, x + 1, at]
                total += field[y, x, before] + field[y, x, after]
                total -= 6.0 * mid
                new = mid + mob[y - 1, x - 1, rows] * total + src[y - 1, x - 1, rows]
                if step < 2:
                    fields[step + 1][y, x, at] = new
                else:
                    end[y - 1, x - 1, rows] = new

    def measure(x):
        for y in range(ny):
            values = end[y, x - 1]
            mean = jnp.sum(values, axis=0, keepdims=True) * (1.0 / nz)
            off = values - mean
            stats[0, x - 1, pl.ds(y, 1)] = mean
            stats[0, x - 1, pl.ds(ny + y, 1)] = jnp.sum(off * off, axis=0, keepdims=True)

    def finish(x):
        for y in range(ny):
            means = [stats[j, x - 1, pl.ds(y, 1)] for j in range(n_down)]
            mean = sum(means[1:], means[0]) * (1.0 / n_down)
            squares = stats[0, x - 1, pl.ds(ny + y, 1)]
            for j in range(1, n_down):
                squares += stats[j, x - 1, pl.ds(ny + y, 1)]
            for value in means:
                squares += nz * ((value - mean) * (value - mean))
            scale = lax.rsqrt(squares * (1.0 / (nz * n_down)) + EPS)
            for z in range(0, nz, ROWS):
                rows = pl.ds(z, ROWS)
                standardized[y, x - 1, rows] = (end[y, x - 1, rows] - mean) * scale

    def over_middle(work):
        @pl.loop(2, nx)
        def _(x):
            work(x)

    def received(copies):
        for copy in copies:
            copy.wait_recv()

    loads[0].wait()
    start([faces[0][0]])
    loads[1].wait()
    start([faces[0][1]])
    loads[2].wait()
    for group in range(3):
        start(edges[0][group])
    loads[3].wait()
    loads[4].wait()
    for group in range(3):
        received(edges[0][group])
    over_middle(functools.partial(column, 0))
    start(edges[1][0])

    received([faces[0][0]])
    column(0, nx)
    start([faces[1][1]])
    start(edges[1][2])

    received([faces[0][1]])
    column(0, 1)
    start([faces[1][0]])
    start(edges[1][1])

    received(edges[1][0])
    over_middle(functools.partial(column, 1))
    start(edges[2][0])

    received([faces[1][1]])
    received(edges[1][1])
    column(1, 1)
    start([faces[2][0]])
    start(edges[2][1])

    received([faces[1][0]])
    received(edges[1][2])
    column(1, nx)
    start([faces[2][1]])
    start(edges[2][2])

    def last(x):
        column(2, x)
        measure(x)

    received(edges[2][0])
    over_middle(last)
    start(spread_moments[0])
    received(spread_moments[0])
    over_middle(finish)

    received([faces[2][0]])
    received(edges[2][2])
    last(nx)
    start(spread_moments[2])
    received(spread_moments[2])
    finish(nx)

    received([faces[2][1]])
    received(edges[2][1])
    last(1)
    start(spread_moments[1])
    received(spread_moments[1])
    finish(1)

    for copy in started:
        copy.wait_send()


def solution(mesh):
    counts = {axis: mesh.shape[axis] for axis in ("south", "east", "down")}
    spec = P(("trial", "south"), "east", "down", None)

    def body(tracer, mobility, source):
        ny, nx, nz, levels = tracer.shape
        block = jax.ShapeDtypeStruct(tracer.shape, tracer.dtype)
        padded = pltpu.VMEM((ny + 2, nx + 2, nz + 2 * PAD, levels), jnp.float32)
        held = pltpu.VMEM(tracer.shape, jnp.float32)
        n_down = counts["down"]
        dma = pltpu.SemaphoreType.DMA
        return pl.pallas_call(
            functools.partial(kernel, counts),
            out_shape=(block, block),
            in_specs=[pl.BlockSpec(memory_space=pl.ANY)] * 3,
            out_specs=[pl.BlockSpec(memory_space=pltpu.VMEM)] * 2,
            scratch_shapes=[
                padded, padded, padded, held, held,
                pltpu.VMEM((n_down, nx, 2 * ny, levels), jnp.float32),
                dma((5,)),
                dma((3, 2)), dma((3, 2)),
                dma((3, 2, 3)), dma((3, 2, 3)),
                dma((3, 2, 3)), dma((3, 2, 3)),
                dma((n_down - 1, 3)), dma((n_down - 1, 3)),
            ],
            compiler_params=pltpu.CompilerParams(
                collective_id=0, has_side_effects=True, vmem_limit_bytes=60 * 1024 * 1024
            ),
        )(tracer, mobility, source)

    return jax.shard_map(
        body, mesh=mesh, in_specs=(spec,) * 3, out_specs=(spec,) * 2, check_vma=False
    )
```

```python
import functools

import jax
import jax.numpy as jnp
from jax import lax
from jax.experimental import pallas as pl
from jax.experimental.pallas import tpu as pltpu
from jax.sharding import PartitionSpec as P

MESH = pl.DeviceIdType.MESH
PAD = 8
ROWS = 32
EPS = 0.0001


def kernel(
    counts, tracer, mobility, source, standardized, end,
    t0, t1, t2, mob, src, stats,
    load_sem, x_send, x_recv, y_send, y_recv, z_send, z_recv, s_send, s_recv,
):
    ny, nx, nz, _ = mob.shape
    n_down = counts["down"]
    me = {axis: lax.axis_index(axis) for axis in counts}

    def peer(axis, offset):
        count = counts[axis]
        return {axis: lax.rem(me[axis] + (offset % count), count)}

    fields = (t0, t1, t2)
    line = pl.ds(PAD, nz)
    low, high, middle = (pl.ds(1, 1), pl.ds(nx, 1), pl.ds(2, nx - 2))
    groups = (middle, low, high)

    def load(sem, array, into):
        return pltpu.make_async_copy(array, into, load_sem.at[sem])

    def load_field(sem, columns):
        inside = pl.ds(columns.start - 1, columns.size)
        return load(sem, tracer.at[:, inside], t0.at[pl.ds(1, ny), columns, line])

    loads = [load_field(i, c) for i, c in enumerate((low, high, middle))]
    loads += [load(3, mobility, mob), load(4, source, src)]
    for copy in loads:
        copy.start()

    def send(field, from_, to, sems, at, device):
        return pltpu.make_async_remote_copy(
            src_ref=field.at[from_],
            dst_ref=field.at[to],
            send_sem=sems[0].at[at],
            recv_sem=sems[1].at[at],
            device_id=device,
            device_id_type=MESH,
        )

    inner_y = pl.ds(1, ny)

    def face(step, side):
        from_, to, offset = ((1, nx + 1, -1), (nx, 0, 1))[side]
        return send(
            fields[step],
            (inner_y, pl.ds(from_, 1), line),
            (inner_y, pl.ds(to, 1), line),
            (x_send, x_recv), (step, side), peer("east", offset),
        )

    def borders(step, group):
        columns = groups[group]
        field = fields[step]
        copies = []
        for side, (from_, to, offset) in enumerate(((1, ny + 1, -1), (ny, 0, 1))):
            copies.append(send(
                field, (pl.ds(from_, 1), columns, line), (pl.ds(to, 1), columns, line),
                (y_send, y_recv), (step, side, group), peer("south", offset),
            ))
        for side, (from_, to, offset) in enumerate(
            ((PAD, PAD + nz, -1), (PAD + nz - 1, PAD - 1, 1))
        ):
            copies.append(send(
                field, (inner_y, columns, pl.ds(from_, 1)), (inner_y, columns, pl.ds(to, 1)),
                (z_send, z_recv), (step, side, group), peer("down", offset),
            ))
        return copies

    def moments(group):
        columns = groups[group]
        inside = pl.ds(columns.start - 1, columns.size)
        return [
            pltpu.make_async_remote_copy(
                src_ref=stats.at[0, inside],
                dst_ref=stats.at[j, inside],
                send_sem=s_send.at[j - 1, group],
                recv_sem=s_recv.at[j - 1, group],
                device_id=peer("down", j),
                device_id_type=MESH,
            )
            for j in range(1, n_down)
        ]

    started = []

    def start(copies):
        for copy in copies:
            copy.start()
            started.append(copy)

    barrier = pltpu.get_barrier_semaphore()
    greeted = [peer("south", -1), peer("south", 1), peer("east", -1), peer("east", 1)]
    greeted += [peer("down", j) for j in range(1, n_down)]
    for device in greeted:
        pl.semaphore_signal(barrier, inc=1, device_id=device, device_id_type=MESH)
    pl.semaphore_wait(barrier, len(greeted))

    faces = [[face(step, side) for side in (0, 1)] for step in range(3)]
    edges = [[borders(step, group) for group in range(3)] for step in range(3)]
    spread_moments = [moments(group) for group in range(3)]

    def column(step, x):
        field = fields[step]
        for z in range(0, nz, ROWS):
            at = pl.ds(PAD + z, ROWS)
            before, after = pl.ds(PAD + z - 1, ROWS), pl.ds(PAD + z + 1, ROWS)
            rows = pl.ds(z, ROWS)
            lines = [field[y, x, at] for y in range(ny + 2)]
            for y in range(1, ny + 1):
                mid = lines[y]
                total = lines[y - 1] + lines[y + 1]
                total += field[y, x - 1, at] + field[y, x + 1, at]
                total += field[y, x, before] + field[y, x, after]
                total -= 6.0 * mid
                new = mid + mob[y - 1, x - 1, rows] * total + src[y - 1, x - 1, rows]
                if step < 2:
                    fields[step + 1][y, x, at] = new
                else:
                    end[y - 1, x - 1, rows] = new

    def measure(x):
        for y in range(ny):
            values = end[y, x - 1]
            mean = jnp.sum(values, axis=0, keepdims=True) * (1.0 / nz)
            off = values - mean
            stats[0, x - 1, pl.ds(y, 1)] = mean
            stats[0, x - 1, pl.ds(ny + y, 1)] = jnp.sum(off * off, axis=0, keepdims=True)

    def finish(x):
        for y in range(ny):
            means = [stats[j, x - 1, pl.ds(y, 1)] for j in range(n_down)]
            mean = sum(means[1:], means[0]) * (1.0 / n_down)
            squares = stats[0, x - 1, pl.ds(ny + y, 1)]
            for j in range(1, n_down):
                squares += stats[j, x - 1, pl.ds(ny + y, 1)]
            for value in means:
                squares += nz * ((value - mean) * (value - mean))
            scale = lax.rsqrt(squares * (1.0 / (nz * n_down)) + EPS)
            for z in range(0, nz, ROWS):
                rows = pl.ds(z, ROWS)
                standardized[y, x - 1, rows] = (end[y, x - 1, rows] - mean) * scale

    def over_middle(work):
        @pl.loop(2, nx)
        def _(x):
            work(x)

    def received(copies):
        for copy in copies:
            copy.wait_recv()

    loads[0].wait()
    start([faces[0][0]])
    loads[1].wait()
    start([faces[0][1]])
    loads[2].wait()
    for group in range(3):
        start(edges[0][group])
    loads[3].wait()
    loads[4].wait()
    for group in range(3):
        received(edges[0][group])
    over_middle(functools.partial(column, 0))
    start(edges[1][0])

    received([faces[0][0]])
    column(0, nx)
    start([faces[1][1]])
    start(edges[1][2])

    received([faces[0][1]])
    column(0, 1)
    start([faces[1][0]])
    start(edges[1][1])

    received(edges[1][0])
    over_middle(functools.partial(column, 1))
    start(edges[2][0])

    received([faces[1][1]])
    received(edges[1][1])
    column(1, 1)
    start([faces[2][0]])
    start(edges[2][1])

    received([faces[1][0]])
    received(edges[1][2])
    column(1, nx)
    start([faces[2][1]])
    start(edges[2][2])

    def last(x):
        column(2, x)
        measure(x)

    received(edges[2][0])
    over_middle(last)
    start(spread_moments[0])
    received(spread_moments[0])
    over_middle(finish)

    received([faces[2][0]])
    received(edges[2][2])
    last(nx)
    start(spread_moments[2])
    received(spread_moments[2])
    finish(nx)

    received([faces[2][1]])
    received(edges[2][1])
    last(1)
    start(spread_moments[1])
    received(spread_moments[1])
    finish(1)

    for copy in started:
        copy.wait_send()


def write_out(standardized, end, standardized_out, end_out, sem):
    pairs = ((standardized, standardized_out), (end, end_out))
    copies = [
        pltpu.make_async_copy(held.at[y], out.at[y], sem.at[i, y])
        for y in range(end.shape[0])
        for i, (held, out) in enumerate(pairs)
    ]
    for copy in copies:
        copy.start()
    for copy in copies:
        copy.wait()


def solution(mesh):
    counts = {axis: mesh.shape[axis] for axis in ("south", "east", "down")}
    spec = P(("trial", "south"), "east", "down", None)

    def body(tracer, mobility, source):
        ny, nx, nz, levels = tracer.shape
        block = pltpu.VMEM(tracer.shape, tracer.dtype)
        padded = pltpu.VMEM((ny + 2, nx + 2, nz + 2 * PAD, levels), jnp.float32)
        held = pltpu.VMEM(tracer.shape, jnp.float32)
        n_down = counts["down"]
        dma = pltpu.SemaphoreType.DMA
        held_outputs = pl.pallas_call(
            functools.partial(kernel, counts),
            out_shape=(block, block),
            in_specs=[pl.BlockSpec(memory_space=pltpu.HBM)] * 3,
            out_specs=[pl.BlockSpec(memory_space=pltpu.VMEM)] * 2,
            scratch_shapes=[
                padded, padded, padded, held, held,
                pltpu.VMEM((n_down, nx, 2 * ny, levels), jnp.float32),
                dma((5,)),
                dma((3, 2)), dma((3, 2)),
                dma((3, 2, 3)), dma((3, 2, 3)),
                dma((3, 2, 3)), dma((3, 2, 3)),
                dma((n_down - 1, 3)), dma((n_down - 1, 3)),
            ],
            compiler_params=pltpu.CompilerParams(
                collective_id=0, has_side_effects=True, vmem_limit_bytes=54 * 1024 * 1024
            ),
        )(tracer, mobility, source)
        return pl.pallas_call(
            write_out,
            out_shape=(pltpu.HBM(tracer.shape, tracer.dtype),) * 2,
            in_specs=[pl.BlockSpec(memory_space=pltpu.VMEM)] * 2,
            out_specs=[pl.BlockSpec(memory_space=pltpu.HBM)] * 2,
            scratch_shapes=[dma((2, ny))],
            compiler_params=pltpu.CompilerParams(vmem_limit_bytes=40 * 1024 * 1024),
        )(*[pltpu.with_memory_space_constraint(held, pltpu.VMEM) for held in held_outputs])

    return jax.shard_map(
        body, mesh=mesh, in_specs=(spec,) * 3, out_specs=(spec,) * 2, check_vma=False
    )
```

```python
import functools

import jax
import jax.numpy as jnp
from jax import lax
from jax.experimental import pallas as pl
from jax.experimental.pallas import tpu as pltpu
from jax.sharding import PartitionSpec as P

MESH = pl.DeviceIdType.MESH
PAD = 8
ROWS = 32
EPS = 0.0001
HOLD = 1


def kernel(
    counts, tracer, mobility, source, standardized, end,
    t0, t1, t2, mob, src, stats,
    load_sem, x_send, x_recv, y_send, y_recv, z_send, z_recv, s_send, s_recv,
):
    ny, nx, nz, _ = mob.shape
    n_down = counts["down"]
    me = {axis: lax.axis_index(axis) for axis in counts}

    def peer(axis, offset):
        count = counts[axis]
        return {axis: lax.rem(me[axis] + (offset % count), count)}

    fields = (t0, t1, t2)
    line = pl.ds(PAD, nz)
    low, high, middle = (pl.ds(1, 1), pl.ds(nx, 1), pl.ds(2, nx - 2))
    groups = (middle, low, high)

    def load(sem, array, into):
        return pltpu.make_async_copy(array, into, load_sem.at[sem])

    def load_field(sem, columns):
        inside = pl.ds(columns.start - 1, columns.size)
        return load(sem, tracer.at[:, inside], t0.at[pl.ds(1, ny), columns, line])

    loads = [load_field(i, c) for i, c in enumerate((low, high, middle))]
    loads += [load(3, mobility, mob), load(4, source, src)]
    for copy in loads:
        copy.start()

    def send(field, from_, to, sems, at, device):
        return pltpu.make_async_remote_copy(
            src_ref=field.at[from_],
            dst_ref=field.at[to],
            send_sem=sems[0].at[at],
            recv_sem=sems[1].at[at],
            device_id=device,
            device_id_type=MESH,
        )

    inner_y = pl.ds(1, ny)

    def face(step, side):
        from_, to, offset = ((1, nx + 1, -1), (nx, 0, 1))[side]
        return [
            send(
                fields[step],
                (inner_y, pl.ds(from_, 1), line),
                (inner_y, pl.ds(to, 1), line),
                (x_send, x_recv), (step, side), peer("east", offset),
            )
        ]

    def borders(step, group):
        columns = groups[group]
        field = fields[step]
        copies = []
        for side, (from_, to, offset) in enumerate(((1, ny + 1, -1), (ny, 0, 1))):
            copies.append(send(
                field, (pl.ds(from_, 1), columns, line), (pl.ds(to, 1), columns, line),
                (y_send, y_recv), (step, side, group), peer("south", offset),
            ))
        for side, (from_, to, offset) in enumerate(
            ((PAD, PAD + nz, -1), (PAD + nz - 1, PAD - 1, 1))
        ):
            copies.append(send(
                field, (inner_y, columns, pl.ds(from_, 1)), (inner_y, columns, pl.ds(to, 1)),
                (z_send, z_recv), (step, side, group), peer("down", offset),
            ))
        return copies

    def moments(columns, at):
        inside = pl.ds(columns.start - 1, columns.size)
        return [
            pltpu.make_async_remote_copy(
                src_ref=stats.at[0, inside],
                dst_ref=stats.at[j, inside],
                send_sem=s_send.at[j - 1, at],
                recv_sem=s_recv.at[j - 1, at],
                device_id=peer("down", j),
                device_id_type=MESH,
            )
            for j in range(1, n_down)
        ]

    started = []

    def start(copies):
        for copy in copies:
            copy.start()
            started.append(copy)

    barrier = pltpu.get_barrier_semaphore()
    greeted = [peer("south", -1), peer("south", 1), peer("east", -1), peer("east", 1)]
    greeted += [peer("down", j) for j in range(1, n_down)]
    for device in greeted:
        pl.semaphore_signal(barrier, inc=1, device_id=device, device_id_type=MESH)
    pl.semaphore_wait(barrier, len(greeted))

    faces = [[face(step, side) for side in (0, 1)] for step in range(3)]
    edges = [[borders(step, group) for group in range(3)] for step in range(3)]
    middle_moments, low_moments, high_moments = [
        moments(columns, at) for at, columns in enumerate(groups)
    ]

    def column(step, x):
        field = fields[step]
        for z in range(0, nz, ROWS):
            at = pl.ds(PAD + z, ROWS)
            before, after = pl.ds(PAD + z - 1, ROWS), pl.ds(PAD + z + 1, ROWS)
            rows = pl.ds(z, ROWS)
            lines = [field[y, x, at] for y in range(ny + 2)]
            for y in range(1, ny + 1):
                mid = lines[y]
                total = lines[y - 1] + lines[y + 1]
                total += field[y, x - 1, at] + field[y, x + 1, at]
                total += field[y, x, before] + field[y, x, after]
                total -= 6.0 * mid
                new = mid + mob[y - 1, x - 1, rows] * total + src[y - 1, x - 1, rows]
                if step < 2:
                    fields[step + 1][y, x, at] = new
                else:
                    end[y - 1, x - 1, rows] = new

    def measure(x):
        for y in range(ny):
            values = end[y, x - 1]
            mean = jnp.sum(values, axis=0, keepdims=True) * (1.0 / nz)
            off = values - mean
            stats[0, x - 1, pl.ds(2 * y, 1)] = mean
            stats[0, x - 1, pl.ds(2 * y + 1, 1)] = jnp.sum(off * off, axis=0, keepdims=True)

    def finish(x):
        for y in range(ny):
            means = [stats[j, x - 1, pl.ds(2 * y, 1)] for j in range(n_down)]
            mean = sum(means[1:], means[0]) * (1.0 / n_down)
            squares = stats[0, x - 1, pl.ds(2 * y + 1, 1)]
            for j in range(1, n_down):
                squares += stats[j, x - 1, pl.ds(2 * y + 1, 1)]
            for value in means:
                squares += nz * ((value - mean) * (value - mean))
            scale = lax.rsqrt(squares * (1.0 / (nz * n_down)) + EPS)
            for z in range(0, nz, ROWS):
                rows = pl.ds(z, ROWS)
                standardized[y, x - 1, rows] = (end[y, x - 1, rows] - mean) * scale

    def over_middle(work):
        @pl.loop(2, nx)
        def _(x):
            work(x)

    def received(copies):
        for copy in copies:
            copy.wait_recv()

    loads[0].wait()
    loads[1].wait()
    ahead = lax.rem(me["south"], 2) == 0
    both = faces[0][0] + faces[0][1]
    started.extend(both)

    @pl.when(ahead)
    def _():
        for copy in both:
            copy.start()

    loads[2].wait()
    for group in (1, 2, 0):
        start(edges[0][group])
    received(edges[0][1][:HOLD])

    @pl.when(jnp.logical_not(ahead))
    def _():
        for copy in both:
            copy.start()

    loads[3].wait()
    loads[4].wait()
    received(edges[0][1][HOLD:] + edges[0][2] + edges[0][0])
    over_middle(functools.partial(column, 0))
    start(edges[1][0])

    received(faces[0][0])
    column(0, nx)
    start(faces[1][1])
    start(edges[1][2])

    received(faces[0][1])
    column(0, 1)
    start(faces[1][0])
    start(edges[1][1])

    received(edges[1][0])
    over_middle(functools.partial(column, 1))
    start(edges[2][0])

    received(faces[1][1])
    received(edges[1][1])
    column(1, 1)
    start(faces[2][0])
    start(edges[2][1])

    received(faces[1][0])
    received(edges[1][2])
    column(1, nx)
    start(faces[2][1])
    start(edges[2][2])

    def last(x):
        column(2, x)
        measure(x)

    received(edges[2][0])
    over_middle(last)
    start(middle_moments)
    received(middle_moments)
    over_middle(finish)

    def last_edge(x, arriving, travelling):
        received(arriving)
        last(x)
        start(travelling)
        received(travelling)
        finish(x)

    received(edges[2][2])
    last_edge(nx, faces[2][0], high_moments)
    received(edges[2][1])
    last_edge(1, faces[2][1], low_moments)

    for copy in started:
        copy.wait_send()


def write_out(standardized, end, standardized_out, end_out, sem):
    pairs = ((standardized, standardized_out), (end, end_out))
    copies = [
        pltpu.make_async_copy(held.at[y], out.at[y], sem.at[i, y])
        for y in range(end.shape[0])
        for i, (held, out) in enumerate(pairs)
    ]
    for copy in copies:
        copy.start()
    for copy in copies:
        copy.wait()


def solution(mesh):
    counts = {axis: mesh.shape[axis] for axis in ("south", "east", "down")}
    spec = P(("trial", "south"), "east", "down", None)

    def body(tracer, mobility, source):
        ny, nx, nz, levels = tracer.shape
        block = pltpu.VMEM(tracer.shape, tracer.dtype)
        padded = pltpu.VMEM((ny + 2, nx + 2, nz + 2 * PAD, levels), jnp.float32)
        held = pltpu.VMEM(tracer.shape, jnp.float32)
        n_down = counts["down"]
        dma = pltpu.SemaphoreType.DMA
        held_outputs = pl.pallas_call(
            functools.partial(kernel, counts),
            out_shape=(block, block),
            in_specs=[pl.BlockSpec(memory_space=pltpu.HBM)] * 3,
            out_specs=[pl.BlockSpec(memory_space=pltpu.VMEM)] * 2,
            scratch_shapes=[
                padded, padded, padded, held, held,
                pltpu.VMEM((n_down, nx, 2 * ny, levels), jnp.float32),
                dma((5,)),
                dma((3, 2)), dma((3, 2)),
                dma((3, 2, 3)), dma((3, 2, 3)),
                dma((3, 2, 3)), dma((3, 2, 3)),
                dma((n_down - 1, 3)), dma((n_down - 1, 3)),
            ],
            compiler_params=pltpu.CompilerParams(
                collective_id=0, has_side_effects=True, vmem_limit_bytes=54 * 1024 * 1024
            ),
        )(tracer, mobility, source)
        return pl.pallas_call(
            write_out,
            out_shape=(pltpu.HBM(tracer.shape, tracer.dtype),) * 2,
            in_specs=[pl.BlockSpec(memory_space=pltpu.VMEM)] * 2,
            out_specs=[pl.BlockSpec(memory_space=pltpu.HBM)] * 2,
            scratch_shapes=[dma((2, ny))],
            compiler_params=pltpu.CompilerParams(vmem_limit_bytes=40 * 1024 * 1024),
        )(*[pltpu.with_memory_space_constraint(held, pltpu.VMEM) for held in held_outputs])

    return jax.shard_map(
        body, mesh=mesh, in_specs=(spec,) * 3, out_specs=(spec,) * 2, check_vma=False
    )
```
